32 devices in a mesh: layer: 2 (over x), blk: 16 (over z, y, core).
Axes of the slice: x: 2, y: 2, z: 4, core: 2. Of those that a mesh axis runs over, the one named last changes fastest.
Arguments:
- sources: bfloat16 [2, 2, 16384, 128], P('layer', None, 'blk'), may hold values from -6 to 6
- near_blocks: bfloat16 [2, 16384, 1024], P('layer', 'blk'), may hold values from -0.09375 to 0.09375
- left_factors: bfloat16 [2, 16384, 512], P('layer', 'blk'), may hold values from -0.125 to 0.125
- right_factors: bfloat16 [2, 16384, 512], P('layer', 'blk'), may hold values from -0.046875 to 0.046875
Outputs:
- traces: bfloat16 [2, 2, 16384, 128], P('layer', None, 'blk')
The draws below stay inside these ranges and needn't reach their ends.
All inputs are finite; a program needn't handle non-finite values.
Results may differ from the reference program's by a relative error of at most 0.014.
Values may be sent and summed in bfloat16 or wider, within the bound.
A program may use at most 64 MiB of HBM per device.

```python
import jax
import jax.numpy as jnp

PB = 1024
RANK = 512
SRCS = 128
BATCHES = 2
POINTS = 16384
LAYERS = 2
N_BLK = 16


def shard_levels(stream_key, dims, split, low, top_value):
    factor_of, own = 1.0, jax.random.fold_in(stream_key, 6)
    for position, blocks in split:
        draws = jnp.exp(jax.random.uniform(jax.random.fold_in(own, position), (blocks,), jnp.float32, low / len(split), top_value / len(split)))
        factor_of = factor_of * jnp.repeat(draws, dims[position] // blocks).reshape([-1 if axis == position else 1 for axis in range(len(dims))])
    return factor_of


def centred(stream_key, shape, scale, limit, pieces=(), held_as=jnp.bfloat16):
    values = jax.random.normal(stream_key, shape, jnp.float32) * scale
    if len(pieces) > 0:
        values = shard_levels(stream_key, shape, pieces, -0.22, 0.18) * values
    return jnp.clip(values, min=-limit, max=limit).astype(held_as)


def setup_inputs(seed: int = 0) -> dict:
    key_list = jax.random.split(jax.random.key(seed), 5)
    return {
        "sources": centred(key_list[0], (LAYERS, BATCHES, POINTS, SRCS), 1.0, 6.0, ((0, 2), (2, 16))),
        "near_blocks": centred(key_list[1], (LAYERS, POINTS, PB), (4 * PB) ** -0.5, 0.09375, ((0, 2), (1, 16))),
        "left_factors": centred(key_list[2], (LAYERS, POINTS, RANK), (4 * RANK) ** -0.5, 0.125, ((0, 2), (1, 16))),
        "right_factors": centred(key_list[3], (LAYERS, POINTS, RANK), POINTS ** -0.5, 0.046875, ((0, 2), (1, 16))),
    }


def reference(sources, near_blocks, left_factors, right_factors):
    results = []
    previous = [None] * BATCHES
    for layer_idx in range(LAYERS):
        blocks = near_blocks[layer_idx].reshape(N_BLK, PB, PB).astype(jnp.float32)
        row = []
        for batch in range(BATCHES):
            total = sources[layer_idx, batch].astype(jnp.float32)
            if previous[batch] is not None:
                total = total + previous[batch].astype(jnp.float32)
            incoming = total.astype(jnp.bfloat16)
            near = jnp.einsum("kpq,kqb->kpb", blocks, incoming.reshape(N_BLK, PB, SRCS).astype(jnp.float32)).reshape(POINTS, SRCS)
            coeff = jnp.dot(right_factors[layer_idx].T, incoming, preferred_element_type=jnp.float32).astype(jnp.bfloat16)
            result = (near + jnp.dot(left_factors[layer_idx], coeff, preferred_element_type=jnp.float32)).astype(jnp.bfloat16)
            row.append(result)
            previous[batch] = result
        results.append(jnp.stack(row))
    return jnp.stack(results)
```

```python
import functools

import jax
import jax.numpy as jnp
from jax import lax
from jax.experimental import pallas as pl
from jax.experimental.pallas import tpu as pltpu
from jax.sharding import PartitionSpec as P

MESH = pl.DeviceIdType.MESH
F32 = jnp.float32
BF16 = jnp.bfloat16


def sweep_kernel(
    layers, blocks, pieces, x_parts,
    src_hbm, near_hbm, left_hbm, right_hbm, out_hbm,
    src, near_w, left_w, right_w, inc, arrived, part, core_in, chip_sum,
    scatter_in, coeff, near, result,
    load_sem, core_send, core_recv, rs_send, rs_recv, ag_send, ag_recv,
    fw_send, fw_recv, x_send, x_recv, out_sem,
):
    layer = lax.axis_index("layer")
    blk = lax.axis_index("blk")
    chips = blocks // 2
    chip, core = blk // 2, lax.rem(blk, 2)
    batches, points, srcs = src.shape
    rank = left_w.shape[1]
    half = rank // 2
    rows = half // pieces
    sub = points // x_parts
    partner = (layer, chip * 2 + (1 - core))

    loads = [
        pltpu.make_async_copy(right_hbm.at[0], right_w, load_sem.at[0]),
        pltpu.make_async_copy(src_hbm.at[0], src, load_sem.at[1]),
        pltpu.make_async_copy(near_hbm.at[0], near_w, load_sem.at[2]),
        pltpu.make_async_copy(left_hbm.at[0], left_w, load_sem.at[3]),
    ]
    for load in loads:
        load.start()

    def peer(i):
        return lax.rem(chip + i, chips)

    barrier = pltpu.get_barrier_semaphore()

    def greet(i, carry):
        pl.semaphore_signal(barrier, inc=1, device_id=(layer, peer(i) * 2 + core), device_id_type=MESH)
        return carry

    lax.fori_loop(1, chips, greet, 0)
    pl.semaphore_signal(barrier, inc=1, device_id=partner, device_id_type=MESH)

    @pl.when(layer > 0)
    def _():
        pl.semaphore_signal(barrier, inc=1, device_id=(layer - 1, blk), device_id_type=MESH)

    @pl.when(layer < layers - 1)
    def _():
        pl.semaphore_signal(barrier, inc=1, device_id=(layer + 1, blk), device_id_type=MESH)

    before = lax.div(layer + layers - 1, layers)
    after = lax.div(2 * layers - 2 - layer, layers)
    pl.semaphore_wait(barrier, chips + before + after)

    def core_copy(b):
        return pltpu.make_async_remote_copy(
            src_ref=part.at[b, pl.ds(pl.multiple_of((1 - core) * half, half), half)],
            dst_ref=core_in.at[b],
            send_sem=core_send.at[b], recv_sem=core_recv.at[b],
            device_id=partner, device_id_type=MESH,
        )

    def rs_copy(b, j):
        return pltpu.make_async_remote_copy(
            src_ref=chip_sum.at[b, pl.ds(pl.multiple_of(j * rows, rows), rows)],
            dst_ref=scatter_in.at[b, chip],
            send_sem=rs_send.at[b, j], recv_sem=rs_recv.at[b, chip],
            device_id=(layer, j * 2 + core), device_id_type=MESH,
        )

    def rs_arrival(b, j):
        return pltpu.make_async_remote_copy(
            src_ref=scatter_in.at[b, j], dst_ref=scatter_in.at[b, j],
            send_sem=rs_send.at[b, j], recv_sem=rs_recv.at[b, j],
            device_id=partner, device_id_type=MESH,
        )

    def piece(b, side, j):
        return coeff.at[b, pl.ds(pl.multiple_of(side * half + j * rows, rows), rows)]

    def ag_copy(b, j):
        return pltpu.make_async_remote_copy(
            src_ref=piece(b, core, chip), dst_ref=piece(b, core, chip),
            send_sem=ag_send.at[b, j], recv_sem=ag_recv.at[b, chip],
            device_id=(layer, j * 2 + core), device_id_type=MESH,
        )

    def ag_arrival(b, j):
        return pltpu.make_async_remote_copy(
            src_ref=piece(b, core, j), dst_ref=piece(b, core, j),
            send_sem=ag_send.at[b, j], recv_sem=ag_recv.at[b, j],
            device_id=partner, device_id_type=MESH,
        )

    def fw_copy(b, j):
        return pltpu.make_async_remote_copy(
            src_ref=piece(b, core, j), dst_ref=piece(b, core, j),
            send_sem=fw_send.at[b, j], recv_sem=fw_recv.at[b, j],
            device_id=partner, device_id_type=MESH,
        )

    def fw_arrival(b, j):
        return pltpu.make_async_remote_copy(
            src_ref=piece(b, 1 - core, j), dst_ref=piece(b, 1 - core, j),
            send_sem=fw_send.at[b, j], recv_sem=fw_recv.at[b, j],
            device_id=partner, device_id_type=MESH,
        )

    def x_copy(b, k):
        return pltpu.make_async_remote_copy(
            src_ref=result.at[b, pl.ds(k * sub, sub)],
            dst_ref=arrived.at[b, pl.ds(k * sub, sub)],
            send_sem=x_send.at[b, k], recv_sem=x_recv.at[b, k],
            device_id=(lax.rem(layer + 1, layers), blk), device_id_type=MESH,
        )

    def out_copy(b):
        return pltpu.make_async_copy(result.at[b], out_hbm.at[0, b], out_sem.at[b])

    owns = chip < pieces

    def each_peer(action, only_owners=False):
        def body(i, carry):
            j = peer(i)
            if only_owners and pieces < chips:
                @pl.when(j < pieces)
                def _():
                    action(j)
            else:
                action(j)
            return carry

        lax.fori_loop(1, chips, body, 0)

    def take_in(b, first):
        if first:
            inc[b] = src[b]
        else:
            for k in range(x_parts):
                x_copy(b, k).wait_recv()
            inc[b] = (src[b].astype(F32) + arrived[b].astype(F32)).astype(BF16)

    def partial_sum(b):
        part[b] = lax.dot_general(
            right_w[...], inc[b], (((0,), (0,)), ((), ())), preferred_element_type=F32
        ).astype(BF16)
        core_copy(b).start()

    def scatter(b):
        core_copy(b).wait_recv()
        mine = part[b, pl.ds(pl.multiple_of(core * half, half), half)]
        chip_sum[b] = (mine.astype(F32) + core_in[b].astype(F32)).astype(BF16)
        each_peer(lambda j: rs_copy(b, j).start(), True)

    def near_product(b):
        near[b] = jnp.dot(near_w[...], inc[b], preferred_element_type=F32)

    def gather(b):
        @pl.when(owns)
        def _():
            each_peer(lambda j: rs_arrival(b, j).wait_recv())
            scatter_in[b, chip] = chip_sum[b, pl.ds(pl.multiple_of(chip * rows, rows), rows)]
            total = jnp.sum(scatter_in[b].astype(F32), axis=0)
            coeff[b, pl.ds(pl.multiple_of(core * half + chip * rows, rows), rows)] = total.astype(BF16)
            each_peer(lambda j: ag_copy(b, j).start())
            fw_copy(b, chip).start()

    def forward(b):
        def pass_on(j):
            ag_arrival(b, j).wait_recv()
            fw_copy(b, j).start()

        each_peer(pass_on, True)

    def finish(b):
        def body(j, carry):
            fw_arrival(b, j).wait_recv()
            return carry

        lax.fori_loop(0, pieces, body, 0)
        for k in range(x_parts):
            at = pl.ds(k * sub, sub)
            result[b, at] = (
                near[b, at] + jnp.dot(left_w[at], coeff[b], preferred_element_type=F32)
            ).astype(BF16)

            @pl.when(layer < layers - 1)
            def _():
                x_copy(b, k).start()

        out_copy(b).start()

    loads[0].wait()
    loads[1].wait()

    every = range(batches)

    @pl.when(layer == 0)
    def _():
        for b in every:
            take_in(b, True)
            partial_sum(b)
        for b in every:
            scatter(b)
        loads[2].wait()
        for b in every:
            near_product(b)
        for b in every:
            gather(b)
        loads[3].wait()
        for b in every:
            forward(b)
        for b in every:
            finish(b)

    @pl.when(layer > 0)
    def _():
        loads[2].wait()
        loads[3].wait()
        for b in every:
            take_in(b, False)
            partial_sum(b)
            scatter(b)
            if b > 0:
                gather(b - 1)
            near_product(b)
            if b > 0:
                forward(b - 1)
        gather(batches - 1)
        for b in range(batches - 1):
            finish(b)
        forward(batches - 1)
        finish(batches - 1)

    for b in every:
        core_copy(b).wait_send()
        each_peer(lambda j: rs_copy(b, j).wait_send(), True)

        @pl.when(owns)
        def _():
            each_peer(lambda j: ag_copy(b, j).wait_send())

        def body(j, carry):
            fw_copy(b, j).wait_send()
            return carry

        lax.fori_loop(0, pieces, body, 0)

        @pl.when(layer < layers - 1)
        def _():
            for k in range(x_parts):
                x_copy(b, k).wait_send()

        out_copy(b).wait()


def solution(mesh):
    layers, blocks = mesh.shape["layer"], mesh.shape["blk"]

    def on_device(sources, near_blocks, left_factors, right_factors):
        _, batches, points, srcs = sources.shape
        rank = left_factors.shape[2]
        half = rank // 2
        chips = blocks // 2
        pieces = min(chips, half // 16)
        rows = half // pieces
        x_parts = 2
        dma = pltpu.SemaphoreType.DMA
        return pl.pallas_call(
            functools.partial(sweep_kernel, layers, blocks, pieces, x_parts),
            out_shape=jax.ShapeDtypeStruct(sources.shape, BF16),
            in_specs=[pl.BlockSpec(memory_space=pl.ANY)] * 4,
            out_specs=pl.BlockSpec(memory_space=pl.ANY),
            scratch_shapes=[
                pltpu.VMEM((batches, points, srcs), BF16),
                pltpu.VMEM(near_blocks.shape[1:], BF16),
                pltpu.VMEM(left_factors.shape[1:], BF16),
                pltpu.VMEM(right_factors.shape[1:], BF16),
                pltpu.VMEM((batches, points, srcs), BF16),
                pltpu.VMEM((batches, points, srcs), BF16),
                pltpu.VMEM((batches, rank, srcs), BF16),
                pltpu.VMEM((batches, half, srcs), BF16),
                pltpu.VMEM((batches, half, srcs), BF16),
                pltpu.VMEM((batches, chips, rows, srcs), BF16),
                pltpu.VMEM((batches, rank, srcs), BF16),
                pltpu.VMEM((batches, points, srcs), F32),
                pltpu.VMEM((batches, points, srcs), BF16),
                dma((4,)),
                dma((batches,)), dma((batches,)),
                dma((batches, chips)), dma((batches, chips)),
                dma((batches, chips)), dma((batches, chips)),
                dma((batches, pieces)), dma((batches, pieces)),
                dma((batches, x_parts)), dma((batches, x_parts)),
                dma((batches,)),
            ],
            compiler_params=pltpu.CompilerParams(collective_id=0, has_side_effects=True),
        )(sources, near_blocks, left_factors, right_factors)

    return jax.shard_map(
        on_device,
        mesh=mesh,
        in_specs=(
            P("layer", None, "blk", None),
            P("layer", "blk", None),
            P("layer", "blk", None),
            P("layer", "blk", None),
        ),
        out_specs=P("layer", None, "blk", None),
        check_vma=False,
    )
```

```python
import functools

import jax
import jax.numpy as jnp
from jax import lax
from jax.experimental import pallas as pl
from jax.experimental.pallas import tpu as pltpu
from jax.sharding import PartitionSpec as P

MESH = pl.DeviceIdType.MESH
F32 = jnp.float32
BF16 = jnp.bfloat16


def sweep_kernel(
    layers, blocks, pieces, split,
    src_hbm, near_hbm, left_hbm, right_hbm, out_hbm,
    src, near_w, left_w, right_w, inc, arrived, part, core_in, chip_sum,
    scatter_in, coeff, near, result,
    next_right, last_left, near_out, near_in, carry_out, carry_in,
    load_sem, core_send, core_recv, rs_send, rs_recv, ag_send, ag_recv,
    fw_send, fw_recv, x_send, x_recv, near_send, near_recv, up_send, up_recv,
    carry_send, carry_recv, factor_send, factor_recv, out_sem,
):
    layer = lax.axis_index("layer")
    blk = lax.axis_index("blk")
    chips = blocks // 2
    chip, core = blk // 2, lax.rem(blk, 2)
    batches, points, srcs = src.shape
    rank = left_w.shape[1]
    half = rank // 2
    rows = half // pieces
    every = range(batches)
    columns = [slice(b * srcs, (b + 1) * srcs) for b in every]
    front, back = pl.ds(0, split), pl.ds(split, points - split)
    partner = (layer, chip * 2 + (1 - core))
    above = (lax.rem(layer + 1, layers), blk)
    below = (lax.rem(layer + layers - 1, layers), blk)
    has_next = layer < layers - 1
    has_last = layer > 0

    loads = [
        pltpu.make_async_copy(right_hbm.at[0], right_w, load_sem.at[0]),
        pltpu.make_async_copy(src_hbm.at[0], src, load_sem.at[1]),
        pltpu.make_async_copy(near_hbm.at[0], near_w, load_sem.at[2]),
        pltpu.make_async_copy(left_hbm.at[0], left_w, load_sem.at[3]),
    ]
    for load in loads:
        load.start()

    def peer(i):
        return lax.rem(chip + i, chips)

    barrier = pltpu.get_barrier_semaphore()

    def greet(i, carry):
        pl.semaphore_signal(barrier, inc=1, device_id=(layer, peer(i) * 2 + core), device_id_type=MESH)
        return carry

    lax.fori_loop(1, chips, greet, 0)
    pl.semaphore_signal(barrier, inc=1, device_id=partner, device_id_type=MESH)

    @pl.when(has_last)
    def _():
        pl.semaphore_signal(barrier, inc=1, device_id=below, device_id_type=MESH)

    @pl.when(has_next)
    def _():
        pl.semaphore_signal(barrier, inc=1, device_id=above, device_id_type=MESH)

    before = lax.div(layer + layers - 1, layers)
    after = lax.div(2 * layers - 2 - layer, layers)
    pl.semaphore_wait(barrier, chips + before + after)

    def remote(src_ref, dst_ref, send_sem, recv_sem, device):
        return pltpu.make_async_remote_copy(
            src_ref=src_ref, dst_ref=dst_ref, send_sem=send_sem, recv_sem=recv_sem,
            device_id=device, device_id_type=MESH,
        )

    def core_copy(n):
        return remote(
            part.at[n, pl.ds(pl.multiple_of((1 - core) * half, half), half)], core_in.at[n],
            core_send.at[n], core_recv.at[n], partner,
        )

    def rs_copy(n, j):
        return remote(
            chip_sum.at[n, pl.ds(pl.multiple_of(j * rows, rows), rows)], scatter_in.at[n, chip],
            rs_send.at[n, j], rs_recv.at[n, chip], (layer, j * 2 + core),
        )

    def rs_arrival(n, j):
        return remote(
            scatter_in.at[n, j], scatter_in.at[n, j], rs_send.at[n, j], rs_recv.at[n, j], partner,
        )

    def piece(n, side, j):
        q, b = divmod(n, batches)
        return coeff.at[
            q, pl.ds(pl.multiple_of(side * half + j * rows, rows), rows), pl.ds(b * srcs, srcs)
        ]

    def ag_copy(n, j):
        own = piece(n, core, chip)
        return remote(own, own, ag_send.at[n, j], ag_recv.at[n, chip], (layer, j * 2 + core))

    def ag_arrival(n, j):
        there = piece(n, core, j)
        return remote(there, there, ag_send.at[n, j], ag_recv.at[n, j], partner)

    def fw_copy(n, j):
        there = piece(n, core, j)
        return remote(there, there, fw_send.at[n, j], fw_recv.at[n, j], partner)

    def fw_arrival(n, j):
        there = piece(n, 1 - core, j)
        return remote(there, there, fw_send.at[n, j], fw_recv.at[n, j], partner)

    def up_copy(b):
        return remote(
            piece(b, core, chip), piece(batches + b, core, chip), up_send.at[b], up_recv.at[b], above
        )

    def carry_copy(b):
        return remote(carry_out.at[b], carry_in.at[b], carry_send.at[b], carry_recv.at[b], above)

    def x_copy(b):
        return remote(result.at[b, front], arrived.at[b], x_send.at[b], x_recv.at[b], above)

    def near_copy(b):
        return remote(near_out.at[b], near_in.at[b], near_send.at[b], near_recv.at[b], above)

    left_copy = remote(
        left_hbm.at[0, back], last_left, factor_send.at[0], factor_recv.at[0], above
    )
    right_copy = remote(
        right_hbm.at[0, front], next_right, factor_send.at[1], factor_recv.at[1], below
    )

    def out_copy(b):
        return pltpu.make_async_copy(result.at[b], out_hbm.at[0, b], out_sem.at[b])

    @pl.when(has_next)
    def _():
        left_copy.start()

    @pl.when(has_last)
    def _():
        right_copy.start()

    owns = chip < pieces

    def each_peer(action, only_owners=False):
        def body(i, carry):
            j = peer(i)
            if only_owners and pieces < chips:
                @pl.when(j < pieces)
                def _():
                    action(j)
            else:
                action(j)
            return carry

        lax.fori_loop(1, chips, body, 0)

    def each_piece(action):
        def body(j, carry):
            action(j)
            return carry

        lax.fori_loop(0, pieces, body, 0)

    def over_points(weights, values):
        return lax.dot_general(weights, values, (((0,), (0,)), ((), ())), preferred_element_type=F32)

    def send_partial(q, value):
        for b in every:
            part[q * batches + b] = value[:, columns[b]].astype(BF16)
            core_copy(q * batches + b).start()

    def scatter(n):
        core_copy(n).wait_recv()
        mine = part[n, pl.ds(pl.multiple_of(core * half, half), half)]
        chip_sum[n] = (mine.astype(F32) + core_in[n].astype(F32)).astype(BF16)
        each_peer(lambda j: rs_copy(n, j).start(), True)

    def piece_total(n):
        each_peer(lambda j: rs_arrival(n, j).wait_recv())
        scatter_in[n, chip] = chip_sum[n, pl.ds(pl.multiple_of(chip * rows, rows), rows)]
        return jnp.sum(scatter_in[n].astype(F32), axis=0)

    def gather(b, first):
        @pl.when(owns)
        def _():
            total = piece_total(b)
            if not first:
                carry_copy(b).wait_recv()
                total = total + carry_in[b].astype(F32)
            coeff[
                0, pl.ds(pl.multiple_of(core * half + chip * rows, rows), rows), columns[b]
            ] = total.astype(BF16)
            each_peer(lambda j: ag_copy(b, j).start())
            fw_copy(b, chip).start()

            @pl.when(has_next)
            def _():
                up_copy(b).start()

    def gather_last(b):
        @pl.when(owns)
        def _():
            up_copy(b).wait_recv()
            each_peer(lambda j: ag_copy(batches + b, j).start())
            fw_copy(batches + b, chip).start()

    def forward(n):
        def pass_on(j):
            ag_arrival(n, j).wait_recv()
            fw_copy(n, j).start()

        each_peer(pass_on, True)

    def near_product(at):
        near[at] = jnp.dot(near_w[at], inc[...], preferred_element_type=F32)

    def send_near():
        @pl.when(has_next)
        def _():
            for b in every:
                near_out[b] = near[back, columns[b]].astype(BF16)
                near_copy(b).start()

    def finish():
        for b in every:
            each_piece(lambda j: fw_arrival(b, j).wait_recv())
        for at in (front, back):
            value = (
                near[at] + jnp.dot(left_w[at], coeff[0], preferred_element_type=F32)
            ).astype(BF16)
            for b in every:
                result[b, at] = value[:, columns[b]]
            if at is front:
                @pl.when(has_next)
                def _():
                    right_copy.wait_recv()
                    send_partial(1, over_points(next_right[...], value))
                    for b in every:
                        x_copy(b).start()
        for b in every:
            out_copy(b).start()

        @pl.when(has_next)
        def _():
            for b in every:
                scatter(batches + b)
            for b in every:
                @pl.when(owns)
                def _():
                    carry_out[b] = piece_total(batches + b).astype(BF16)
                    carry_copy(b).start()

    loads[0].wait()
    loads[1].wait()

    @pl.when(layer == 0)
    def _():
        for b in every:
            inc[:, columns[b]] = src[b]
        send_partial(0, over_points(right_w[...], inc[...]))
        loads[2].wait()
        near_product(back)
        send_near()
        for b in every:
            scatter(b)
        near_product(front)
        for b in every:
            gather(b, True)
        loads[3].wait()
        for b in every:
            forward(b)
        finish()

    @pl.when(has_last)
    def _():
        for b in every:
            inc[front, columns[b]] = src[b, front]
        base = over_points(right_w[front], inc[front])
        loads[2].wait()
        loads[3].wait()
        left_copy.wait_recv()
        for b in every:
            near_copy(b).wait_recv()
        for b in every:
            gather_last(b)
        for b in every:
            forward(batches + b)
        for b in every:
            each_piece(lambda j: fw_arrival(batches + b, j).wait_recv())
        far = jnp.dot(last_left[...], coeff[1], preferred_element_type=F32)
        for b in every:
            trace = (near_in[b].astype(F32) + far[:, columns[b]]).astype(BF16)
            inc[back, columns[b]] = (src[b, back].astype(F32) + trace.astype(F32)).astype(BF16)
        send_partial(0, base + over_points(right_w[back], inc[back]))
        for b in every:
            scatter(b)
        for b in every:
            x_copy(b).wait_recv()
            inc[front, columns[b]] = (
                src[b, front].astype(F32) + arrived[b].astype(F32)
            ).astype(BF16)
        near_product(back)
        send_near()
        near_product(front)
        for b in every:
            gather(b, False)
        for b in every:
            forward(b)
        finish()

    def sent(n):
        core_copy(n).wait_send()
        each_peer(lambda j: rs_copy(n, j).wait_send(), True)

    def gathered(n):
        @pl.when(owns)
        def _():
            each_peer(lambda j: ag_copy(n, j).wait_send())

        each_piece(lambda j: fw_copy(n, j).wait_send())

    for b in every:
        sent(b)
        gathered(b)

        @pl.when(has_last)
        def _():
            gathered(batches + b)

        @pl.when(has_next)
        def _():
            sent(batches + b)
            near_copy(b).wait_send()
            x_copy(b).wait_send()

            @pl.when(owns)
            def _():
                up_copy(b).wait_send()
                carry_copy(b).wait_send()

        out_copy(b).wait()

    @pl.when(has_next)
    def _():
        left_copy.wait_send()

    @pl.when(has_last)
    def _():
        right_copy.wait_send()


def solution(mesh):
    layers, blocks = mesh.shape["layer"], mesh.shape["blk"]

    def on_device(sources, near_blocks, left_factors, right_factors):
        _, batches, points, srcs = sources.shape
        rank = left_factors.shape[2]
        half = rank // 2
        chips = blocks // 2
        pieces = min(chips, half // 16)
        rows = half // pieces
        split = points * 5 // 8
        rest = points - split
        dma = pltpu.SemaphoreType.DMA
        vmem = pltpu.VMEM
        return pl.pallas_call(
            functools.partial(sweep_kernel, layers, blocks, pieces, split),
            out_shape=jax.ShapeDtypeStruct(sources.shape, BF16),
            in_specs=[pl.BlockSpec(memory_space=pl.ANY)] * 4,
            out_specs=pl.BlockSpec(memory_space=pl.ANY),
            scratch_shapes=[
                vmem((batches, points, srcs), BF16),
                vmem(near_blocks.shape[1:], BF16),
                vmem(left_factors.shape[1:], BF16),
                vmem(right_factors.shape[1:], BF16),
                vmem((points, batches * srcs), BF16),
                vmem((batches, split, srcs), BF16),
                vmem((2 * batches, rank, srcs), BF16),
                vmem((2 * batches, half, srcs), BF16),
                vmem((2 * batches, half, srcs), BF16),
                vmem((2 * batches, chips, rows, srcs), BF16),
                vmem((2, rank, batches * srcs), BF16),
                vmem((points, batches * srcs), F32),
                vmem((batches, points, srcs), BF16),
                vmem((split, rank), BF16),
                vmem((rest, rank), BF16),
                vmem((batches, rest, srcs), BF16),
                vmem((batches, rest, srcs), BF16),
                vmem((batches, rows, srcs), BF16),
                vmem((batches, rows, srcs), BF16),
                dma((4,)),
                dma((2 * batches,)), dma((2 * batches,)),
                dma((2 * batches, chips)), dma((2 * batches, chips)),
                dma((2 * batches, chips)), dma((2 * batches, chips)),
                dma((2 * batches, pieces)), dma((2 * batches, pieces)),
                dma((batches,)), dma((batches,)),
                dma((batches,)), dma((batches,)),
                dma((batches,)), dma((batches,)),
                dma((batches,)), dma((batches,)),
                dma((2,)), dma((2,)),
                dma((batches,)),
            ],
            compiler_params=pltpu.CompilerParams(collective_id=0, has_side_effects=True),
        )(sources, near_blocks, left_factors, right_factors)

    return jax.shard_map(
        on_device,
        mesh=mesh,
        in_specs=(
            P("layer", None, "blk", None),
            P("layer", "blk", None),
            P("layer", "blk", None),
            P("layer", "blk", None),
        ),
        out_specs=P("layer", None, "blk", None),
        check_vma=False,
    )
```

```python
import functools

import jax
import jax.numpy as jnp
from jax import lax
from jax.experimental import pallas as pl
from jax.experimental.pallas import tpu as pltpu
from jax.sharding import PartitionSpec as P

MESH = pl.DeviceIdType.MESH
F32 = jnp.float32
BF16 = jnp.bfloat16


def sweep_kernel(
    layers, blocks, pieces, split,
    src_hbm, near_hbm, left_hbm, right_hbm, out_hbm,
    src, near_w, left_w, right_w, inc, arrived, part, core_in, chip_sum,
    scatter_in, coeff, near, result,
    next_right, last_left, near_out, near_in, carry_out, carry_in, base,
    load_sem, core_send, core_recv, rs_send, rs_recv, ag_send, ag_recv,
    fw_send, fw_recv, x_send, x_recv, near_send, near_recv, up_send, up_recv,
    carry_send, carry_recv, factor_send, factor_recv, out_sem,
):
    layer = lax.axis_index("layer")
    blk = lax.axis_index("blk")
    chips = blocks // 2
    chip, core = blk // 2, lax.rem(blk, 2)
    batches, points, srcs = src.shape
    rank = left_w.shape[1]
    half = rank // 2
    rows = half // pieces
    every = range(batches)
    columns = [slice(b * srcs, (b + 1) * srcs) for b in every]
    front, back = pl.ds(0, split), pl.ds(split, points - split)
    partner = (layer, chip * 2 + (1 - core))
    above = (lax.rem(layer + 1, layers), blk)
    below = (lax.rem(layer + layers - 1, layers), blk)
    has_next = layer < layers - 1
    has_last = layer > 0

    loads = [
        pltpu.make_async_copy(right_hbm.at[0], right_w, load_sem.at[0]),
        pltpu.make_async_copy(src_hbm.at[0], src, load_sem.at[1]),
        pltpu.make_async_copy(near_hbm.at[0], near_w, load_sem.at[2]),
        pltpu.make_async_copy(left_hbm.at[0], left_w, load_sem.at[3]),
    ]
    for load in loads:
        load.start()

    def peer(i):
        return lax.rem(chip + i, chips)

    barrier = pltpu.get_barrier_semaphore()

    def greet(i, carry):
        pl.semaphore_signal(barrier, inc=1, device_id=(layer, peer(i) * 2 + core), device_id_type=MESH)
        return carry

    lax.fori_loop(1, chips, greet, 0)
    pl.semaphore_signal(barrier, inc=1, device_id=partner, device_id_type=MESH)

    @pl.when(has_last)
    def _():
        pl.semaphore_signal(barrier, inc=1, device_id=below, device_id_type=MESH)

    @pl.when(has_next)
    def _():
        pl.semaphore_signal(barrier, inc=1, device_id=above, device_id_type=MESH)

    before = lax.div(layer + layers - 1, layers)
    after = lax.div(2 * layers - 2 - layer, layers)

    def over_points(weights, values):
        return lax.dot_general(weights, values, (((0,), (0,)), ((), ())), preferred_element_type=F32)

    loads[0].wait()
    loads[1].wait()

    @pl.when(layer == 0)
    def _():
        for b in every:
            inc[:, columns[b]] = src[b]
        base[...] = over_points(right_w[...], inc[...])

    @pl.when(has_last)
    def _():
        for b in every:
            inc[front, columns[b]] = src[b, front]
        base[...] = over_points(right_w[front], inc[front])

    pl.semaphore_wait(barrier, chips + before + after)

    def remote(src_ref, dst_ref, send_sem, recv_sem, device):
        return pltpu.make_async_remote_copy(
            src_ref=src_ref, dst_ref=dst_ref, send_sem=send_sem, recv_sem=recv_sem,
            device_id=device, device_id_type=MESH,
        )

    def core_copy(n):
        return remote(
            part.at[n, pl.ds(pl.multiple_of((1 - core) * half, half), half)], core_in.at[n],
            core_send.at[n], core_recv.at[n], partner,
        )

    def rs_copy(n, j):
        return remote(
            chip_sum.at[n, pl.ds(pl.multiple_of(j * rows, rows), rows)], scatter_in.at[n, chip],
            rs_send.at[n, j], rs_recv.at[n, chip], (layer, j * 2 + core),
        )

    def rs_arrival(n, j):
        return remote(
            scatter_in.at[n, j], scatter_in.at[n, j], rs_send.at[n, j], rs_recv.at[n, j], partner,
        )

    def piece(n, side, j):
        q, b = divmod(n, batches)
        return coeff.at[
            q, pl.ds(pl.multiple_of(side * half + j * rows, rows), rows), pl.ds(b * srcs, srcs)
        ]

    def ag_copy(n, j):
        own = piece(n, core, chip)
        return remote(own, own, ag_send.at[n, j], ag_recv.at[n, chip], (layer, j * 2 + core))

    def ag_arrival(n, j):
        there = piece(n, core, j)
        return remote(there, there, ag_send.at[n, j], ag_recv.at[n, j], partner)

    def fw_copy(n, j):
        there = piece(n, core, j)
        return remote(there, there, fw_send.at[n, j], fw_recv.at[n, j], partner)

    def fw_arrival(n, j):
        there = piece(n, 1 - core, j)
        return remote(there, there, fw_send.at[n, j], fw_recv.at[n, j], partner)

    def up_copy(b):
        return remote(
            piece(b, core, chip), piece(batches + b, core, chip), up_send.at[b], up_recv.at[b], above
        )

    def carry_copy(b):
        return remote(carry_out.at[b], carry_in.at[b], carry_send.at[b], carry_recv.at[b], above)

    def x_copy(b):
        return remote(result.at[b, front], arrived.at[b], x_send.at[b], x_recv.at[b], above)

    def near_copy(b):
        return remote(near_out.at[b], near_in.at[b], near_send.at[b], near_recv.at[b], above)

    first_rows = points // 4

    def left_copy(k):
        at, size = (0, first_rows) if k == 0 else (first_rows, points - split - first_rows)
        return remote(
            left_hbm.at[0, pl.ds(split + at, size)], last_left.at[pl.ds(at, size)],
            factor_send.at[k], factor_recv.at[k], above,
        )

    right_copy = remote(
        right_hbm.at[0, front], next_right, factor_send.at[2], factor_recv.at[2], below
    )

    def out_copy(b):
        return pltpu.make_async_copy(result.at[b], out_hbm.at[0, b], out_sem.at[b])

    @pl.when(has_next)
    def _():
        left_copy(0).start()

    @pl.when(has_last)
    def _():
        right_copy.start()

    owns = chip < pieces

    def each_peer(action, only_owners=False):
        def body(i, carry):
            j = peer(i)
            if only_owners and pieces < chips:
                @pl.when(j < pieces)
                def _():
                    action(j)
            else:
                action(j)
            return carry

        lax.fori_loop(1, chips, body, 0)

    def each_piece(action):
        def body(j, carry):
            action(j)
            return carry

        lax.fori_loop(0, pieces, body, 0)

    def send_partial(q, value):
        for b in every:
            part[q * batches + b] = value[:, columns[b]].astype(BF16)
            core_copy(q * batches + b).start()

    def scatter(n):
        core_copy(n).wait_recv()
        mine = part[n, pl.ds(pl.multiple_of(core * half, half), half)]
        chip_sum[n] = (mine.astype(F32) + core_in[n].astype(F32)).astype(BF16)
        each_peer(lambda j: rs_copy(n, j).start(), True)

    def piece_total(n):
        each_peer(lambda j: rs_arrival(n, j).wait_recv())
        scatter_in[n, chip] = chip_sum[n, pl.ds(pl.multiple_of(chip * rows, rows), rows)]
        return jnp.sum(scatter_in[n].astype(F32), axis=0)

    def gather(b, first):
        @pl.when(owns)
        def _():
            total = piece_total(b)
            if not first:
                carry_copy(b).wait_recv()
                total = total + carry_in[b].astype(F32)
            coeff[
                0, pl.ds(pl.multiple_of(core * half + chip * rows, rows), rows), columns[b]
            ] = total.astype(BF16)
            each_peer(lambda j: ag_copy(b, j).start())
            fw_copy(b, chip).start()

            @pl.when(has_next)
            def _():
                up_copy(b).start()

    def gather_last(b):
        @pl.when(owns)
        def _():
            up_copy(b).wait_recv()
            each_peer(lambda j: ag_copy(batches + b, j).start())
            fw_copy(batches + b, chip).start()

    def forward(n):
        def pass_on(j):
            ag_arrival(n, j).wait_recv()
            fw_copy(n, j).start()

        each_peer(pass_on, True)

    def near_product(at):
        near[at] = jnp.dot(near_w[at], inc[...], preferred_element_type=F32)

    def send_near():
        @pl.when(has_next)
        def _():
            left_copy(1).start()
            for b in every:
                near_out[b] = near[back, columns[b]].astype(BF16)
                near_copy(b).start()

    def finish():
        for b in every:
            each_piece(lambda j: fw_arrival(b, j).wait_recv())
        for at in (front, back):
            value = (
                near[at] + jnp.dot(left_w[at], coeff[0], preferred_element_type=F32)
            ).astype(BF16)
            for b in every:
                result[b, at] = value[:, columns[b]]
            if at is front:
                @pl.when(has_next)
                def _():
                    right_copy.wait_recv()
                    send_partial(1, over_points(next_right[...], value))
                    for b in every:
                        x_copy(b).start()
        for b in every:
            out_copy(b).start()

        @pl.when(has_next)
        def _():
            for b in every:
                scatter(batches + b)
            for b in every:
                @pl.when(owns)
                def _():
                    carry_out[b] = piece_total(batches + b).astype(BF16)
                    carry_copy(b).start()

    @pl.when(layer == 0)
    def _():
        send_partial(0, base[...])
        loads[2].wait()
        near_product(back)
        for b in every:
            scatter(b)
        near_product(front)
        for b in every:
            gather(b, True)
        send_near()
        loads[3].wait()
        for b in every:
            forward(b)
        finish()

    @pl.when(has_last)
    def _():
        loads[2].wait()
        loads[3].wait()
        left_copy(0).wait_recv()
        for b in every:
            gather_last(b)
        for b in every:
            forward(batches + b)
        left_copy(1).wait_recv()
        for b in every:
            near_copy(b).wait_recv()
        for b in every:
            each_piece(lambda j: fw_arrival(batches + b, j).wait_recv())
        far = jnp.dot(last_left[...], coeff[1], preferred_element_type=F32)
        for b in every:
            trace = (near_in[b].astype(F32) + far[:, columns[b]]).astype(BF16)
            inc[back, columns[b]] = (src[b, back].astype(F32) + trace.astype(F32)).astype(BF16)
        send_partial(0, base[...] + over_points(right_w[back], inc[back]))
        for b in every:
            scatter(b)
        for b in every:
            x_copy(b).wait_recv()
            inc[front, columns[b]] = (
                src[b, front].astype(F32) + arrived[b].astype(F32)
            ).astype(BF16)
        near_product(back)
        near_product(front)
        for b in every:
            gather(b, False)
        send_near()
        for b in every:
            forward(b)
        finish()

    def sent(n):
        core_copy(n).wait_send()
        each_peer(lambda j: rs_copy(n, j).wait_send(), True)

    def gathered(n):
        @pl.when(owns)
        def _():
            each_peer(lambda j: ag_copy(n, j).wait_send())

        each_piece(lambda j: fw_copy(n, j).wait_send())

    for b in every:
        sent(b)
        gathered(b)

        @pl.when(has_last)
        def _():
            gathered(batches + b)

        @pl.when(has_next)
        def _():
            sent(batches + b)
            near_copy(b).wait_send()
            x_copy(b).wait_send()

            @pl.when(owns)
            def _():
                up_copy(b).wait_send()
                carry_copy(b).wait_send()

        out_copy(b).wait()

    @pl.when(has_next)
    def _():
        left_copy(0).wait_send()
        left_copy(1).wait_send()

    @pl.when(has_last)
    def _():
        right_copy.wait_send()


def solution(mesh):
    layers, blocks = mesh.shape["layer"], mesh.shape["blk"]

    def on_device(sources, near_blocks, left_factors, right_factors):
        _, batches, points, srcs = sources.shape
        rank = left_factors.shape[2]
        half = rank // 2
        chips = blocks // 2
        pieces = min(chips, half // 16)
        rows = half // pieces
        split = points * 19 // 32
        rest = points - split
        dma = pltpu.SemaphoreType.DMA
        vmem = pltpu.VMEM
        return pl.pallas_call(
            functools.partial(sweep_kernel, layers, blocks, pieces, split),
            out_shape=jax.ShapeDtypeStruct(sources.shape, BF16),
            in_specs=[pl.BlockSpec(memory_space=pl.ANY)] * 4,
            out_specs=pl.BlockSpec(memory_space=pl.ANY),
            scratch_shapes=[
                vmem((batches, points, srcs), BF16),
                vmem(near_blocks.shape[1:], BF16),
                vmem(left_factors.shape[1:], BF16),
                vmem(right_factors.shape[1:], BF16),
                vmem((points, batches * srcs), BF16),
                vmem((batches, split, srcs), BF16),
                vmem((2 * batches, rank, srcs), BF16),
                vmem((2 * batches, half, srcs), BF16),
                vmem((2 * batches, half, srcs), BF16),
                vmem((2 * batches, chips, rows, srcs), BF16),
                vmem((2, rank, batches * srcs), BF16),
                vmem((points, batches * srcs), F32),
                vmem((batches, points, srcs), BF16),
                vmem((split, rank), BF16),
                vmem((rest, rank), BF16),
                vmem((batches, rest, srcs), BF16),
                vmem((batches, rest, srcs), BF16),
                vmem((batches, rows, srcs), BF16),
                vmem((batches, rows, srcs), BF16),
                vmem((rank, batches * srcs), F32),
                dma((4,)),
                dma((2 * batches,)), dma((2 * batches,)),
                dma((2 * batches, chips)), dma((2 * batches, chips)),
                dma((2 * batches, chips)), dma((2 * batches, chips)),
                dma((2 * batches, pieces)), dma((2 * batches, pieces)),
                dma((batches,)), dma((batches,)),
                dma((batches,)), dma((batches,)),
                dma((batches,)), dma((batches,)),
                dma((batches,)), dma((batches,)),
                dma((3,)), dma((3,)),
                dma((batches,)),
            ],
            compiler_params=pltpu.CompilerParams(collective_id=0, has_side_effects=True),
        )(sources, near_blocks, left_factors, right_factors)

    return jax.shard_map(
        on_device,
        mesh=mesh,
        in_specs=(
            P("layer", None, "blk", None),
            P("layer", "blk", None),
            P("layer", "blk", None),
            P("layer", "blk", None),
        ),
        out_specs=P("layer", None, "blk", None),
        check_vma=False,
    )
```

```python
import functools

import jax
import jax.numpy as jnp
from jax import lax
from jax.experimental import pallas as pl
from jax.experimental.pallas import tpu as pltpu
from jax.sharding import PartitionSpec as P

MESH = pl.DeviceIdType.MESH
F32 = jnp.float32
BF16 = jnp.bfloat16


def sweep_kernel(
    layers, blocks, pieces, split,
    src_hbm, near_hbm, left_hbm, right_hbm, result_block,
    src, near_w, left_w, right_w, inc, arrived, part, core_in, chip_sum,
    scatter_in, coeff, near,
    next_right, last_left, near_out, near_in, carry_out, carry_in, base,
    load_sem, core_send, core_recv, rs_send, rs_recv, ag_send, ag_recv,
    fw_send, fw_recv, x_send, x_recv, near_send, near_recv, up_send, up_recv,
    carry_send, carry_recv, factor_send, factor_recv,
):
    layer = lax.axis_index("layer")
    blk = lax.axis_index("blk")
    chips = blocks // 2
    chip, core = blk // 2, lax.rem(blk, 2)
    batches, points, srcs = src.shape
    result = result_block.at[0]
    rank = left_w.shape[1]
    half = rank // 2
    rows = half // pieces
    every = range(batches)
    columns = [slice(b * srcs, (b + 1) * srcs) for b in every]
    front, back = pl.ds(0, split), pl.ds(split, points - split)
    partner = (layer, chip * 2 + (1 - core))
    above = (lax.rem(layer + 1, layers), blk)
    below = (lax.rem(layer + layers - 1, layers), blk)
    has_next = layer < layers - 1
    has_last = layer > 0

    loads = [
        pltpu.make_async_copy(right_hbm.at[0], right_w, load_sem.at[0]),
        pltpu.make_async_copy(src_hbm.at[0], src, load_sem.at[1]),
        pltpu.make_async_copy(near_hbm.at[0], near_w, load_sem.at[2]),
        pltpu.make_async_copy(left_hbm.at[0], left_w, load_sem.at[3]),
    ]
    for load in loads:
        load.start()

    def peer(i):
        return lax.rem(chip + i, chips)

    barrier = pltpu.get_barrier_semaphore()

    def greet(i, carry):
        pl.semaphore_signal(barrier, inc=1, device_id=(layer, peer(i) * 2 + core), device_id_type=MESH)
        return carry

    lax.fori_loop(1, chips, greet, 0)
    pl.semaphore_signal(barrier, inc=1, device_id=partner, device_id_type=MESH)

    @pl.when(has_last)
    def _():
        pl.semaphore_signal(barrier, inc=1, device_id=below, device_id_type=MESH)

    @pl.when(has_next)
    def _():
        pl.semaphore_signal(barrier, inc=1, device_id=above, device_id_type=MESH)

    before = lax.div(layer + layers - 1, layers)
    after = lax.div(2 * layers - 2 - layer, layers)

    def over_points(weights, values):
        return lax.dot_general(weights, values, (((0,), (0,)), ((), ())), preferred_element_type=F32)

    loads[0].wait()
    loads[1].wait()

    @pl.when(layer == 0)
    def _():
        for b in every:
            inc[:, columns[b]] = src[b]
        base[...] = over_points(right_w[...], inc[...])

    @pl.when(has_last)
    def _():
        for b in every:
            inc[front, columns[b]] = src[b, front]
        base[...] = over_points(right_w[front], inc[front])

    pl.semaphore_wait(barrier, chips + before + after)

    def remote(src_ref, dst_ref, send_sem, recv_sem, device):
        return pltpu.make_async_remote_copy(
            src_ref=src_ref, dst_ref=dst_ref, send_sem=send_sem, recv_sem=recv_sem,
            device_id=device, device_id_type=MESH,
        )

    def core_copy(n):
        return remote(
            part.at[n, pl.ds(pl.multiple_of((1 - core) * half, half), half)], core_in.at[n],
            core_send.at[n], core_recv.at[n], partner,
        )

    def rs_copy(n, j):
        return remote(
            chip_sum.at[n, pl.ds(pl.multiple_of(j * rows, rows), rows)], scatter_in.at[n, chip],
            rs_send.at[n, j], rs_recv.at[n, chip], (layer, j * 2 + core),
        )

    def rs_arrival(n, j):
        return remote(
            scatter_in.at[n, j], scatter_in.at[n, j], rs_send.at[n, j], rs_recv.at[n, j], partner,
        )

    def piece(n, side, j):
        q, b = divmod(n, batches)
        return coeff.at[
            q, pl.ds(pl.multiple_of(side * half + j * rows, rows), rows), pl.ds(b * srcs, srcs)
        ]

    def ag_copy(n, j):
        own = piece(n, core, chip)
        return remote(own, own, ag_send.at[n, j], ag_recv.at[n, chip], (layer, j * 2 + core))

    def ag_arrival(n, j):
        there = piece(n, core, j)
        return remote(there, there, ag_send.at[n, j], ag_recv.at[n, j], partner)

    def fw_copy(n, j):
        there = piece(n, core, j)
        return remote(there, there, fw_send.at[n, j], fw_recv.at[n, j], partner)

    def fw_arrival(n, j):
        there = piece(n, 1 - core, j)
        return remote(there, there, fw_send.at[n, j], fw_recv.at[n, j], partner)

    def up_copy(b):
        return remote(
            piece(b, core, chip), piece(batches + b, core, chip), up_send.at[b], up_recv.at[b], above
        )

    def carry_copy(b):
        return remote(carry_out.at[b], carry_in.at[b], carry_send.at[b], carry_recv.at[b], above)

    def x_copy(b):
        return remote(result.at[b, front], arrived.at[b], x_send.at[b], x_recv.at[b], above)

    def near_copy(b):
        return remote(near_out.at[b], near_in.at[b], near_send.at[b], near_recv.at[b], above)

    first_rows = points // 4

    def left_copy(k):
        at, size = (0, first_rows) if k == 0 else (first_rows, points - split - first_rows)
        return remote(
            left_hbm.at[0, pl.ds(split + at, size)], last_left.at[pl.ds(at, size)],
            factor_send.at[k], factor_recv.at[k], above,
        )

    right_copy = remote(
        right_hbm.at[0, front], next_right, factor_send.at[2], factor_recv.at[2], below
    )

    @pl.when(has_next)
    def _():
        left_copy(0).start()

    @pl.when(has_last)
    def _():
        right_copy.start()

    owns = chip < pieces

    def each_peer(action, only_owners=False):
        def body(i, carry):
            j = peer(i)
            if only_owners and pieces < chips:
                @pl.when(j < pieces)
                def _():
                    action(j)
            else:
                action(j)
            return carry

        lax.fori_loop(1, chips, body, 0)

    def each_piece(action):
        def body(j, carry):
            action(j)
            return carry

        lax.fori_loop(0, pieces, body, 0)

    def send_partial(q, value):
        for b in every:
            part[q * batches + b] = value[:, columns[b]].astype(BF16)
            core_copy(q * batches + b).start()

    def scatter(n):
        core_copy(n).wait_recv()
        mine = part[n, pl.ds(pl.multiple_of(core * half, half), half)]
        chip_sum[n] = (mine.astype(F32) + core_in[n].astype(F32)).astype(BF16)
        each_peer(lambda j: rs_copy(n, j).start(), True)

    def piece_total(n):
        each_peer(lambda j: rs_arrival(n, j).wait_recv())
        scatter_in[n, chip] = chip_sum[n, pl.ds(pl.multiple_of(chip * rows, rows), rows)]
        return jnp.sum(scatter_in[n].astype(F32), axis=0)

    def gather(b, first):
        @pl.when(owns)
        def _():
            total = piece_total(b)
            if not first:
                carry_copy(b).wait_recv()
                total = total + carry_in[b].astype(F32)
            coeff[
                0, pl.ds(pl.multiple_of(core * half + chip * rows, rows), rows), columns[b]
            ] = total.astype(BF16)
            each_peer(lambda j: ag_copy(b, j).start())
            fw_copy(b, chip).start()

            @pl.when(has_next)
            def _():
                up_copy(b).start()

    def gather_last(b):
        @pl.when(owns)
        def _():
            up_copy(b).wait_recv()
            each_peer(lambda j: ag_copy(batches + b, j).start())
            fw_copy(batches + b, chip).start()

    def forward(n):
        def pass_on(j):
            ag_arrival(n, j).wait_recv()
            fw_copy(n, j).start()

        each_peer(pass_on, True)

    def near_product(at):
        near[at] = jnp.dot(near_w[at], inc[...], preferred_element_type=F32)

    def send_near():
        @pl.when(has_next)
        def _():
            left_copy(1).start()
            for b in every:
                near_out[b] = near[back, columns[b]].astype(BF16)
                near_copy(b).start()

    def finish():
        for b in every:
            each_piece(lambda j: fw_arrival(b, j).wait_recv())
        for at in (front, back):
            value = (
                near[at] + jnp.dot(left_w[at], coeff[0], preferred_element_type=F32)
            ).astype(BF16)
            for b in every:
                result[b, at] = value[:, columns[b]]
            if at is front:
                @pl.when(has_next)
                def _():
                    right_copy.wait_recv()
                    send_partial(1, over_points(next_right[...], value))
                    for b in every:
                        x_copy(b).start()
        @pl.when(has_next)
        def _():
            for b in every:
                scatter(batches + b)
            for b in every:
                @pl.when(owns)
                def _():
                    carry_out[b] = piece_total(batches + b).astype(BF16)
                    carry_copy(b).start()

    @pl.when(layer == 0)
    def _():
        send_partial(0, base[...])
        loads[2].wait()
        near_product(back)
        for b in every:
            scatter(b)
        near_product(front)
        for b in every:
            gather(b, True)
        send_near()
        loads[3].wait()
        for b in every:
            forward(b)
        finish()

    @pl.when(has_last)
    def _():
        loads[2].wait()
        loads[3].wait()
        left_copy(0).wait_recv()
        for b in every:
            gather_last(b)
        for b in every:
            forward(batches + b)
        left_copy(1).wait_recv()
        for b in every:
            near_copy(b).wait_recv()
        for b in every:
            each_piece(lambda j: fw_arrival(batches + b, j).wait_recv())
        far = jnp.dot(last_left[...], coeff[1], preferred_element_type=F32)
        for b in every:
            trace = (near_in[b].astype(F32) + far[:, columns[b]]).astype(BF16)
            inc[back, columns[b]] = (src[b, back].astype(F32) + trace.astype(F32)).astype(BF16)
        send_partial(0, base[...] + over_points(right_w[back], inc[back]))
        for b in every:
            scatter(b)
        for b in every:
            x_copy(b).wait_recv()
            inc[front, columns[b]] = (
                src[b, front].astype(F32) + arrived[b].astype(F32)
            ).astype(BF16)
        near_product(back)
        near_product(front)
        for b in every:
            gather(b, False)
        send_near()
        for b in every:
            forward(b)
        finish()

    def sent(n):
        core_copy(n).wait_send()
        each_peer(lambda j: rs_copy(n, j).wait_send(), True)

    def gathered(n):
        @pl.when(owns)
        def _():
            each_peer(lambda j: ag_copy(n, j).wait_send())

        each_piece(lambda j: fw_copy(n, j).wait_send())

    for b in every:
        sent(b)
        gathered(b)

        @pl.when(has_last)
        def _():
            gathered(batches + b)

        @pl.when(has_next)
        def _():
            sent(batches + b)
            near_copy(b).wait_send()
            x_copy(b).wait_send()

            @pl.when(owns)
            def _():
                up_copy(b).wait_send()
                carry_copy(b).wait_send()


    @pl.when(has_next)
    def _():
        left_copy(0).wait_send()
        left_copy(1).wait_send()

    @pl.when(has_last)
    def _():
        right_copy.wait_send()


def solution(mesh):
    layers, blocks = mesh.shape["layer"], mesh.shape["blk"]

    def on_device(sources, near_blocks, left_factors, right_factors):
        _, batches, points, srcs = sources.shape
        rank = left_factors.shape[2]
        half = rank // 2
        chips = blocks // 2
        pieces = min(chips, half // 16)
        rows = half // pieces
        split = points * 19 // 32
        rest = points - split
        dma = pltpu.SemaphoreType.DMA
        vmem = pltpu.VMEM
        return pl.pallas_call(
            functools.partial(sweep_kernel, layers, blocks, pieces, split),
            out_shape=jax.ShapeDtypeStruct(sources.shape, BF16),
            in_specs=[pl.BlockSpec(memory_space=pltpu.HBM)] * 4,
            out_specs=pl.BlockSpec(memory_space=pltpu.VMEM),
            scratch_shapes=[
                vmem((batches, points, srcs), BF16),
                vmem(near_blocks.shape[1:], BF16),
                vmem(left_factors.shape[1:], BF16),
                vmem(right_factors.shape[1:], BF16),
                vmem((points, batches * srcs), BF16),
                vmem((batches, split, srcs), BF16),
                vmem((2 * batches, rank, srcs), BF16),
                vmem((2 * batches, half, srcs), BF16),
                vmem((2 * batches, half, srcs), BF16),
                vmem((2 * batches, chips, rows, srcs), BF16),
                vmem((2, rank, batches * srcs), BF16),
                vmem((points, batches * srcs), F32),
                vmem((split, rank), BF16),
                vmem((rest, rank), BF16),
                vmem((batches, rest, srcs), BF16),
                vmem((batches, rest, srcs), BF16),
                vmem((batches, rows, srcs), BF16),
                vmem((batches, rows, srcs), BF16),
                vmem((rank, batches * srcs), F32),
                dma((4,)),
                dma((2 * batches,)), dma((2 * batches,)),
                dma((2 * batches, chips)), dma((2 * batches, chips)),
                dma((2 * batches, chips)), dma((2 * batches, chips)),
                dma((2 * batches, pieces)), dma((2 * batches, pieces)),
                dma((batches,)), dma((batches,)),
                dma((batches,)), dma((batches,)),
                dma((batches,)), dma((batches,)),
                dma((batches,)), dma((batches,)),
                dma((3,)), dma((3,)),
            ],
            compiler_params=pltpu.CompilerParams(collective_id=0, has_side_effects=True, vmem_limit_bytes=40000000),
        )(*[pltpu.with_memory_space_constraint(a, pltpu.HBM) for a in (sources, near_blocks, left_factors, right_factors)])

    return jax.shard_map(
        on_device,
        mesh=mesh,
        in_specs=(
            P("layer", None, "blk", None),
            P("layer", "blk", None),
            P("layer", "blk", None),
            P("layer", "blk", None),
        ),
        out_specs=P("layer", None, "blk", None),
        check_vma=False,
    )
```

```python
import functools

import jax
import jax.numpy as jnp
from jax import lax
from jax.experimental import pallas as pl
from jax.experimental.pallas import tpu as pltpu
from jax.sharding import PartitionSpec as P

MESH = pl.DeviceIdType.MESH
F32 = jnp.float32
BF16 = jnp.bfloat16


def sweep_kernel(
    layers, blocks, pieces, split,
    src_hbm, near_hbm, left_hbm, right_hbm, result_block,
    src, near_w, left_w, right_w, inc, arrived, part, core_in, chip_sum,
    scatter_in, coeff, near,
    next_right, last_left, near_out, near_in, carry_out, carry_in, base,
    load_sem, core_send, core_recv, rs_send, rs_recv, ag_send, ag_recv,
    fw_send, fw_recv, x_send, x_recv, near_send, near_recv, up_send, up_recv,
    carry_send, carry_recv, factor_send, factor_recv,
):
    layer = lax.axis_index("layer")
    blk = lax.axis_index("blk")
    chips = blocks // 2
    chip, core = blk // 2, lax.rem(blk, 2)
    batches, points, srcs = src.shape
    result = result_block.at[0]
    rank = left_w.shape[1]
    half = rank // 2
    rows = half // pieces
    every = range(batches)
    columns = [slice(b * srcs, (b + 1) * srcs) for b in every]
    front, back = pl.ds(0, split), pl.ds(split, points - split)
    partner = (layer, chip * 2 + (1 - core))
    above = (lax.rem(layer + 1, layers), blk)
    below = (lax.rem(layer + layers - 1, layers), blk)
    has_next = layer < layers - 1
    has_last = layer > 0

    loads = [
        pltpu.make_async_copy(right_hbm.at[0], right_w, load_sem.at[0]),
        pltpu.make_async_copy(src_hbm.at[0], src, load_sem.at[1]),
        pltpu.make_async_copy(near_hbm.at[0], near_w, load_sem.at[2]),
        pltpu.make_async_copy(left_hbm.at[0], left_w, load_sem.at[3]),
    ]
    for load in loads:
        load.start()

    def peer(i):
        return lax.rem(chip + i, chips)

    barrier = pltpu.get_barrier_semaphore()

    def greet(i, carry):
        pl.semaphore_signal(barrier, inc=1, device_id=(layer, peer(i) * 2 + core), device_id_type=MESH)
        return carry

    lax.fori_loop(1, chips, greet, 0)
    pl.semaphore_signal(barrier, inc=1, device_id=partner, device_id_type=MESH)

    @pl.when(has_last)
    def _():
        pl.semaphore_signal(barrier, inc=1, device_id=below, device_id_type=MESH)

    @pl.when(has_next)
    def _():
        pl.semaphore_signal(barrier, inc=1, device_id=above, device_id_type=MESH)

    before = lax.div(layer + layers - 1, layers)
    after = lax.div(2 * layers - 2 - layer, layers)

    def over_points(weights, values):
        return lax.dot_general(weights, values, (((0,), (0,)), ((), ())), preferred_element_type=F32)

    loads[0].wait()
    loads[1].wait()

    @pl.when(layer == 0)
    def _():
        for b in every:
            inc[:, columns[b]] = src[b]
        base[...] = over_points(right_w[...], inc[...])

    @pl.when(has_last)
    def _():
        for b in every:
            inc[front, columns[b]] = src[b, front]
        base[...] = over_points(right_w[front], inc[front])

    pl.semaphore_wait(barrier, chips + before + after)

    def remote(src_ref, dst_ref, send_sem, recv_sem, device):
        return pltpu.make_async_remote_copy(
            src_ref=src_ref, dst_ref=dst_ref, send_sem=send_sem, recv_sem=recv_sem,
            device_id=device, device_id_type=MESH,
        )

    def core_copy(n):
        return remote(
            part.at[n, pl.ds(pl.multiple_of((1 - core) * half, half), half)], core_in.at[n],
            core_send.at[n], core_recv.at[n], partner,
        )

    def rs_copy(n, j):
        return remote(
            chip_sum.at[n, pl.ds(pl.multiple_of(j * rows, rows), rows)], scatter_in.at[n, chip],
            rs_send.at[n, j], rs_recv.at[n, chip], (layer, j * 2 + core),
        )

    def rs_arrival(n, j):
        return remote(
            scatter_in.at[n, j], scatter_in.at[n, j], rs_send.at[n, j], rs_recv.at[n, j], partner,
        )

    def piece(n, side, j):
        q, b = divmod(n, batches)
        return coeff.at[
            q, pl.ds(pl.multiple_of(side * half + j * rows, rows), rows), pl.ds(b * srcs, srcs)
        ]

    def ag_copy(n, j):
        own = piece(n, core, chip)
        return remote(own, own, ag_send.at[n, j], ag_recv.at[n, chip], (layer, j * 2 + core))

    def ag_arrival(n, j):
        there = piece(n, core, j)
        return remote(there, there, ag_send.at[n, j], ag_recv.at[n, j], partner)

    def fw_copy(n, j):
        there = piece(n, core, j)
        return remote(there, there, fw_send.at[n, j], fw_recv.at[n, j], partner)

    def fw_arrival(n, j):
        there = piece(n, 1 - core, j)
        return remote(there, there, fw_send.at[n, j], fw_recv.at[n, j], partner)

    def up_copy(b):
        return remote(
            piece(b, core, chip), piece(batches + b, core, chip), up_send.at[b], up_recv.at[b], above
        )

    def carry_copy(b):
        return remote(carry_out.at[b], carry_in.at[b], carry_send.at[b], carry_recv.at[b], above)

    def x_copy(b):
        return remote(result.at[b, front], arrived.at[b], x_send.at[b], x_recv.at[b], above)

    def near_copy(b):
        return remote(near_out.at[b], near_in.at[b], near_send.at[b], near_recv.at[b], above)

    first_rows = points // 4

    def left_copy(k):
        at, size = (0, first_rows) if k == 0 else (first_rows, points - split - first_rows)
        return remote(
            left_hbm.at[0, pl.ds(split + at, size)], last_left.at[pl.ds(at, size)],
            factor_send.at[k], factor_recv.at[k], above,
        )

    right_copy = remote(
        right_hbm.at[0, front], next_right, factor_send.at[2], factor_recv.at[2], below
    )

    @pl.when(has_next)
    def _():
        left_copy(0).start()

    @pl.when(has_last)
    def _():
        right_copy.start()

    owns = chip < pieces

    def each_peer(action, only_owners=False, nearest=False):
        def body(i, carry):
            k = chips - 2 - i if nearest else i
            j = peer(chips // 2 + (k + 1) // 2 * (2 * lax.rem(k, 2) - 1))
            if only_owners and pieces < chips:
                @pl.when(j < pieces)
                def _():
                    action(j)
            else:
                action(j)
            return carry

        lax.fori_loop(0, chips - 1, body, 0)

    def each_piece(action):
        def body(j, carry):
            action(j)
            return carry

        lax.fori_loop(0, pieces, body, 0)

    def send_partial(q, value):
        for b in every:
            part[q * batches + b] = value[:, columns[b]].astype(BF16)
            core_copy(q * batches + b).start()

    def scatter(n):
        core_copy(n).wait_recv()
        mine = part[n, pl.ds(pl.multiple_of(core * half, half), half)]
        chip_sum[n] = (mine.astype(F32) + core_in[n].astype(F32)).astype(BF16)
        each_peer(lambda j: rs_copy(n, j).start(), True)

    def piece_total(n):
        each_peer(lambda j: rs_arrival(n, j).wait_recv())
        scatter_in[n, chip] = chip_sum[n, pl.ds(pl.multiple_of(chip * rows, rows), rows)]
        return jnp.sum(scatter_in[n].astype(F32), axis=0)

    def gather(b, first):
        @pl.when(owns)
        def _():
            total = piece_total(b)
            if not first:
                carry_copy(b).wait_recv()
                total = total + carry_in[b].astype(F32)
            coeff[
                0, pl.ds(pl.multiple_of(core * half + chip * rows, rows), rows), columns[b]
            ] = total.astype(BF16)
            each_peer(lambda j: ag_copy(b, j).start())
            fw_copy(b, chip).start()

            @pl.when(has_next)
            def _():
                up_copy(b).start()

    def gather_last(b):
        @pl.when(owns)
        def _():
            up_copy(b).wait_recv()
            each_peer(lambda j: ag_copy(batches + b, j).start())
            fw_copy(batches + b, chip).start()

    def forward(n):
        def pass_on(j):
            ag_arrival(n, j).wait_recv()
            fw_copy(n, j).start()

        each_peer(pass_on, True, True)

    def near_product(at):
        near[at] = jnp.dot(near_w[at], inc[...], preferred_element_type=F32)

    def send_near():
        @pl.when(has_next)
        def _():
            left_copy(1).start()
            for b in every:
                near_out[b] = near[back, columns[b]].astype(BF16)
                near_copy(b).start()

    def finish():
        for b in every:
            each_piece(lambda j: fw_arrival(b, j).wait_recv())
        for at in (front, back):
            value = (
                near[at] + jnp.dot(left_w[at], coeff[0], preferred_element_type=F32)
            ).astype(BF16)
            for b in every:
                result[b, at] = value[:, columns[b]]
            if at is front:
                @pl.when(has_next)
                def _():
                    right_copy.wait_recv()
                    send_partial(1, over_points(next_right[...], value))
                    for b in every:
                        x_copy(b).start()
        @pl.when(has_next)
        def _():
            for b in every:
                scatter(batches + b)
            for b in every:
                @pl.when(owns)
                def _():
                    carry_out[b] = piece_total(batches + b).astype(BF16)
                    carry_copy(b).start()

    @pl.when(layer == 0)
    def _():
        send_partial(0, base[...])
        loads[2].wait()
        near_product(back)
        for b in every:
            scatter(b)
        near_product(front)
        for b in every:
            gather(b, True)
        send_near()
        loads[3].wait()
        for b in every:
            forward(b)
        finish()

    @pl.when(has_last)
    def _():
        loads[2].wait()
        loads[3].wait()
        left_copy(0).wait_recv()
        for b in every:
            gather_last(b)
        for b in every:
            forward(batches + b)
        left_copy(1).wait_recv()
        for b in every:
            near_copy(b).wait_recv()
        for b in every:
            each_piece(lambda j: fw_arrival(batches + b, j).wait_recv())
        far = jnp.dot(last_left[...], coeff[1], preferred_element_type=F32)
        for b in every:
            trace = (near_in[b].astype(F32) + far[:, columns[b]]).astype(BF16)
            inc[back, columns[b]] = (src[b, back].astype(F32) + trace.astype(F32)).astype(BF16)
        send_partial(0, base[...] + over_points(right_w[back], inc[back]))
        for b in every:
            scatter(b)
        for b in every:
            gather(b, False)
        for b in every:
            x_copy(b).wait_recv()
            inc[front, columns[b]] = (
                src[b, front].astype(F32) + arrived[b].astype(F32)
            ).astype(BF16)
        near_product(back)
        near_product(front)
        send_near()
        for b in every:
            forward(b)
        finish()

    def sent(n):
        core_copy(n).wait_send()
        each_peer(lambda j: rs_copy(n, j).wait_send(), True)

    def gathered(n):
        @pl.when(owns)
        def _():
            each_peer(lambda j: ag_copy(n, j).wait_send())

        each_piece(lambda j: fw_copy(n, j).wait_send())

    for b in every:
        sent(b)
        gathered(b)

        @pl.when(has_last)
        def _():
            gathered(batches + b)

        @pl.when(has_next)
        def _():
            sent(batches + b)
            near_copy(b).wait_send()
            x_copy(b).wait_send()

            @pl.when(owns)
            def _():
                up_copy(b).wait_send()
                carry_copy(b).wait_send()


    @pl.when(has_next)
    def _():
        left_copy(0).wait_send()
        left_copy(1).wait_send()

    @pl.when(has_last)
    def _():
        right_copy.wait_send()


def solution(mesh):
    layers, blocks = mesh.shape["layer"], mesh.shape["blk"]

    def on_device(sources, near_blocks, left_factors, right_factors):
        _, batches, points, srcs = sources.shape
        rank = left_factors.shape[2]
        half = rank // 2
        chips = blocks // 2
        pieces = min(chips, half // 16)
        rows = half // pieces
        split = points * 19 // 32
        rest = points - split
        dma = pltpu.SemaphoreType.DMA
        vmem = pltpu.VMEM
        return pl.pallas_call(
            functools.partial(sweep_kernel, layers, blocks, pieces, split),
            out_shape=jax.ShapeDtypeStruct(sources.shape, BF16),
            in_specs=[pl.BlockSpec(memory_space=pltpu.HBM)] * 4,
            out_specs=pl.BlockSpec(memory_space=pltpu.VMEM),
            scratch_shapes=[
                vmem((batches, points, srcs), BF16),
                vmem(near_blocks.shape[1:], BF16),
                vmem(left_factors.shape[1:], BF16),
                vmem(right_factors.shape[1:], BF16),
                vmem((points, batches * srcs), BF16),
                vmem((batches, split, srcs), BF16),
                vmem((2 * batches, rank, srcs), BF16),
                vmem((2 * batches, half, srcs), BF16),
                vmem((2 * batches, half, srcs), BF16),
                vmem((2 * batches, chips, rows, srcs), BF16),
                vmem((2, rank, batches * srcs), BF16),
                vmem((points, batches * srcs), F32),
                vmem((split, rank), BF16),
                vmem((rest, rank), BF16),
                vmem((batches, rest, srcs), BF16),
                vmem((batches, rest, srcs), BF16),
                vmem((batches, rows, srcs), BF16),
                vmem((batches, rows, srcs), BF16),
                vmem((rank, batches * srcs), F32),
                dma((4,)),
                dma((2 * batches,)), dma((2 * batches,)),
                dma((2 * batches, chips)), dma((2 * batches, chips)),
                dma((2 * batches, chips)), dma((2 * batches, chips)),
                dma((2 * batches, pieces)), dma((2 * batches, pieces)),
                dma((batches,)), dma((batches,)),
                dma((batches,)), dma((batches,)),
                dma((batches,)), dma((batches,)),
                dma((batches,)), dma((batches,)),
                dma((3,)), dma((3,)),
            ],
            compiler_params=pltpu.CompilerParams(collective_id=0, has_side_effects=True, vmem_limit_bytes=40000000),
        )(*[pltpu.with_memory_space_constraint(a, pltpu.HBM) for a in (sources, near_blocks, left_factors, right_factors)])

    return jax.shard_map(
        on_device,
        mesh=mesh,
        in_specs=(
            P("layer", None, "blk", None),
            P("layer", "blk", None),
            P("layer", "blk", None),
            P("layer", "blk", None),
        ),
        out_specs=P("layer", None, "blk", None),
        check_vma=False,
    )
```

```python
import functools

import jax
import jax.numpy as jnp
from jax import lax
from jax.experimental import pallas as pl
from jax.experimental.pallas import tpu as pltpu
from jax.sharding import PartitionSpec as P

MESH = pl.DeviceIdType.MESH
F32 = jnp.float32
BF16 = jnp.bfloat16


def sweep_kernel(
    layers, blocks, pieces, split,
    src_hbm, near_hbm, left_hbm, right_hbm, result_block,
    src, near_w, left_w, right_w, inc, arrived, part, core_in, chip_sum,
    scatter_in, coeff, near,
    next_right, last_left, near_out, near_in, carry_out, carry_in, base,
    load_sem, core_send, core_recv, rs_send, rs_recv, ag_send, ag_recv,
    fw_send, fw_recv, x_send, x_recv, near_send, near_recv, up_send, up_recv,
    carry_send, carry_recv, factor_send, factor_recv,
):
    layer = lax.axis_index("layer")
    blk = lax.axis_index("blk")
    chips = blocks // 2
    chip, core = blk // 2, lax.rem(blk, 2)
    batches, points, srcs = src.shape
    result = result_block.at[0]
    rank = left_w.shape[1]
    half = rank // 2
    rows = half // pieces
    every = range(batches)
    groups = coeff.shape[0] // 2
    width = coeff.shape[2]
    each_group = range(groups)
    lanes = [slice(g * width, (g + 1) * width) for g in each_group]
    columns = [slice(b * srcs, (b + 1) * srcs) for b in every]
    front, back = pl.ds(0, split), pl.ds(split, points - split)
    partner = (layer, chip * 2 + (1 - core))
    above = (lax.rem(layer + 1, layers), blk)
    below = (lax.rem(layer + layers - 1, layers), blk)
    has_next = layer < layers - 1
    has_last = layer > 0

    loads = [
        pltpu.make_async_copy(right_hbm.at[0], right_w, load_sem.at[0]),
        pltpu.make_async_copy(src_hbm.at[0], src, load_sem.at[1]),
        pltpu.make_async_copy(near_hbm.at[0], near_w, load_sem.at[2]),
        pltpu.make_async_copy(left_hbm.at[0], left_w, load_sem.at[3]),
    ]
    for load in loads:
        load.start()

    def peer(i):
        return lax.rem(chip + i, chips)

    barrier = pltpu.get_barrier_semaphore()

    def greet(i, carry):
        pl.semaphore_signal(barrier, inc=1, device_id=(layer, peer(i) * 2 + core), device_id_type=MESH)
        return carry

    lax.fori_loop(1, chips, greet, 0)
    pl.semaphore_signal(barrier, inc=1, device_id=partner, device_id_type=MESH)

    @pl.when(has_last)
    def _():
        pl.semaphore_signal(barrier, inc=1, device_id=below, device_id_type=MESH)

    @pl.when(has_next)
    def _():
        pl.semaphore_signal(barrier, inc=1, device_id=above, device_id_type=MESH)

    before = lax.div(layer + layers - 1, layers)
    after = lax.div(2 * layers - 2 - layer, layers)

    def over_points(weights, values):
        return lax.dot_general(weights, values, (((0,), (0,)), ((), ())), preferred_element_type=F32)

    loads[0].wait()
    loads[1].wait()

    @pl.when(layer == 0)
    def _():
        for b in every:
            inc[:, columns[b]] = src[b]
        base[...] = over_points(right_w[...], inc[...])

    @pl.when(has_last)
    def _():
        for b in every:
            inc[front, columns[b]] = src[b, front]
        base[...] = over_points(right_w[front], inc[front])

    pl.semaphore_wait(barrier, chips + before + after)

    def remote(src_ref, dst_ref, send_sem, recv_sem, device):
        return pltpu.make_async_remote_copy(
            src_ref=src_ref, dst_ref=dst_ref, send_sem=send_sem, recv_sem=recv_sem,
            device_id=device, device_id_type=MESH,
        )

    def core_copy(n):
        return remote(
            part.at[n, pl.ds(pl.multiple_of((1 - core) * half, half), half)], core_in.at[n],
            core_send.at[n], core_recv.at[n], partner,
        )

    def rs_copy(n, j):
        return remote(
            chip_sum.at[n, pl.ds(pl.multiple_of(j * rows, rows), rows)], scatter_in.at[n, chip],
            rs_send.at[n, j], rs_recv.at[n, chip], (layer, j * 2 + core),
        )

    def rs_arrival(n, j):
        return remote(
            scatter_in.at[n, j], scatter_in.at[n, j], rs_send.at[n, j], rs_recv.at[n, j], partner,
        )

    def piece(n, side, j):
        return coeff.at[n, pl.ds(pl.multiple_of(side * half + j * rows, rows), rows)]

    def ag_copy(n, j):
        own = piece(n, core, chip)
        return remote(own, own, ag_send.at[n, j], ag_recv.at[n, chip], (layer, j * 2 + core))

    def ag_arrival(n, j):
        there = piece(n, core, j)
        return remote(there, there, ag_send.at[n, j], ag_recv.at[n, j], partner)

    def fw_copy(n, j):
        there = piece(n, core, j)
        return remote(there, there, fw_send.at[n, j], fw_recv.at[n, j], partner)

    def fw_arrival(n, j):
        there = piece(n, 1 - core, j)
        return remote(there, there, fw_send.at[n, j], fw_recv.at[n, j], partner)

    def up_copy(b):
        return remote(
            piece(b, core, chip), piece(groups + b, core, chip), up_send.at[b], up_recv.at[b], above
        )

    def carry_copy(b):
        return remote(carry_out.at[b], carry_in.at[b], carry_send.at[b], carry_recv.at[b], above)

    def x_copy(b):
        return remote(result.at[b, front], arrived.at[b], x_send.at[b], x_recv.at[b], above)

    def near_copy(b):
        return remote(near_out.at[b], near_in.at[b], near_send.at[b], near_recv.at[b], above)

    first_rows = points // 4

    def left_copy(k):
        at, size = (0, first_rows) if k == 0 else (first_rows, points - split - first_rows)
        return remote(
            left_hbm.at[0, pl.ds(split + at, size)], last_left.at[pl.ds(at, size)],
            factor_send.at[k], factor_recv.at[k], above,
        )

    right_copy = remote(
        right_hbm.at[0, front], next_right, factor_send.at[2], factor_recv.at[2], below
    )

    @pl.when(has_next)
    def _():
        left_copy(0).start()

    @pl.when(has_last)
    def _():
        right_copy.start()

    owns = chip < pieces

    def each_peer(action, only_owners=False, nearest=False):
        def body(i, carry):
            k = chips - 2 - i if nearest else i
            j = peer(i + 1)
            if only_owners and pieces < chips:
                @pl.when(j < pieces)
                def _():
                    action(j)
            else:
                action(j)
            return carry

        lax.fori_loop(0, chips - 1, body, 0)

    def each_piece(action):
        def body(j, carry):
            action(j)
            return carry

        lax.fori_loop(0, pieces, body, 0)

    def send_partial(q, value):
        for b in each_group:
            part[q * groups + b] = value[:, lanes[b]].astype(BF16)
            core_copy(q * groups + b).start()

    def scatter(n):
        core_copy(n).wait_recv()
        mine = part[n, pl.ds(pl.multiple_of(core * half, half), half)]
        chip_sum[n] = (mine.astype(F32) + core_in[n].astype(F32)).astype(BF16)
        each_peer(lambda j: rs_copy(n, j).start(), True)

    def piece_total(n):
        each_peer(lambda j: rs_arrival(n, j).wait_recv())
        scatter_in[n, chip] = chip_sum[n, pl.ds(pl.multiple_of(chip * rows, rows), rows)]
        return jnp.sum(scatter_in[n].astype(F32), axis=0)

    def gather(b, first):
        @pl.when(owns)
        def _():
            total = piece_total(b)
            if not first:
                carry_copy(b).wait_recv()
                total = total + carry_in[b].astype(F32)
            coeff[b, pl.ds(pl.multiple_of(core * half + chip * rows, rows), rows)] = total.astype(BF16)
            each_peer(lambda j: ag_copy(b, j).start())
            fw_copy(b, chip).start()

            @pl.when(has_next)
            def _():
                up_copy(b).start()

    def gather_last(b):
        @pl.when(owns)
        def _():
            up_copy(b).wait_recv()
            each_peer(lambda j: ag_copy(groups + b, j).start())
            fw_copy(groups + b, chip).start()

    def forward(n):
        def pass_on(j):
            ag_arrival(n, j).wait_recv()
            fw_copy(n, j).start()

        each_peer(pass_on, True, True)

    def near_product(at):
        near[at] = jnp.dot(near_w[at], inc[...], preferred_element_type=F32)

    def send_near():
        @pl.when(has_next)
        def _():
            left_copy(1).start()
            for b in every:
                near_out[b] = near[back, columns[b]].astype(BF16)
                near_copy(b).start()

    def finish():
        for b in each_group:
            each_piece(lambda j: fw_arrival(b, j).wait_recv())
        for at in (front, back):
            value = (
                near[at] + jnp.dot(left_w[at], coeff[0], preferred_element_type=F32)
            ).astype(BF16)
            for b in every:
                result[b, at] = value[:, columns[b]]
            if at is front:
                @pl.when(has_next)
                def _():
                    right_copy.wait_recv()
                    send_partial(1, over_points(next_right[...], value))
                    for b in every:
                        x_copy(b).start()
        @pl.when(has_next)
        def _():
            for b in each_group:
                scatter(groups + b)
            for b in each_group:
                @pl.when(owns)
                def _():
                    carry_out[b] = piece_total(groups + b).astype(BF16)
                    carry_copy(b).start()

    @pl.when(layer == 0)
    def _():
        send_partial(0, base[...])
        loads[2].wait()
        near_product(back)
        for b in each_group:
            scatter(b)
        near_product(front)
        for b in each_group:
            gather(b, True)
        send_near()
        loads[3].wait()
        for b in each_group:
            forward(b)
        finish()

    @pl.when(has_last)
    def _():
        loads[2].wait()
        loads[3].wait()
        left_copy(0).wait_recv()
        for b in each_group:
            gather_last(b)
        for b in each_group:
            forward(groups + b)
        left_copy(1).wait_recv()
        for b in every:
            near_copy(b).wait_recv()
        for b in each_group:
            each_piece(lambda j: fw_arrival(groups + b, j).wait_recv())
        far = jnp.dot(last_left[...], coeff[groups], preferred_element_type=F32)
        for b in every:
            trace = (near_in[b].astype(F32) + far[:, columns[b]]).astype(BF16)
            inc[back, columns[b]] = (src[b, back].astype(F32) + trace.astype(F32)).astype(BF16)
        send_partial(0, base[...] + over_points(right_w[back], inc[back]))
        for b in each_group:
            scatter(b)
        for b in each_group:
            gather(b, False)
        for b in every:
            x_copy(b).wait_recv()
            inc[front, columns[b]] = (
                src[b, front].astype(F32) + arrived[b].astype(F32)
            ).astype(BF16)
        near_product(back)
        near_product(front)
        send_near()
        for b in each_group:
            forward(b)
        finish()

    def sent(n):
        core_copy(n).wait_send()
        each_peer(lambda j: rs_copy(n, j).wait_send(), True)

    def gathered(n):
        @pl.when(owns)
        def _():
            each_peer(lambda j: ag_copy(n, j).wait_send())

        each_piece(lambda j: fw_copy(n, j).wait_send())

    for b in each_group:
        sent(b)
        gathered(b)

        @pl.when(has_last)
        def _():
            gathered(groups + b)

        @pl.when(has_next)
        def _():
            sent(groups + b)

            @pl.when(owns)
            def _():
                up_copy(b).wait_send()
                carry_copy(b).wait_send()

    @pl.when(has_next)
    def _():
        for b in every:
            near_copy(b).wait_send()
            x_copy(b).wait_send()
        left_copy(0).wait_send()
        left_copy(1).wait_send()

    @pl.when(has_last)
    def _():
        right_copy.wait_send()


def solution(mesh):
    layers, blocks = mesh.shape["layer"], mesh.shape["blk"]

    def on_device(sources, near_blocks, left_factors, right_factors):
        _, batches, points, srcs = sources.shape
        rank = left_factors.shape[2]
        half = rank // 2
        chips = blocks // 2
        pieces = min(chips, half // 16)
        rows = half // pieces
        split = points * 19 // 32
        rest = points - split
        groups, width = 1, batches * srcs
        dma = pltpu.SemaphoreType.DMA
        vmem = pltpu.VMEM
        return pl.pallas_call(
            functools.partial(sweep_kernel, layers, blocks, pieces, split),
            out_shape=jax.ShapeDtypeStruct(sources.shape, BF16),
            in_specs=[pl.BlockSpec(memory_space=pltpu.HBM)] * 4,
            out_specs=pl.BlockSpec(memory_space=pltpu.VMEM),
            scratch_shapes=[
                vmem((batches, points, srcs), BF16),
                vmem(near_blocks.shape[1:], BF16),
                vmem(left_factors.shape[1:], BF16),
                vmem(right_factors.shape[1:], BF16),
                vmem((points, batches * srcs), BF16),
                vmem((batches, split, srcs), BF16),
                vmem((2 * groups, rank, width), BF16),
                vmem((2 * groups, half, width), BF16),
                vmem((2 * groups, half, width), BF16),
                vmem((2 * groups, chips, rows, width), BF16),
                vmem((2 * groups, rank, width), BF16),
                vmem((points, batches * srcs), F32),
                vmem((split, rank), BF16),
                vmem((rest, rank), BF16),
                vmem((batches, rest, srcs), BF16),
                vmem((batches, rest, srcs), BF16),
                vmem((groups, rows, width), BF16),
                vmem((groups, rows, width), BF16),
                vmem((rank, batches * srcs), F32),
                dma((4,)),
                dma((2 * groups,)), dma((2 * groups,)),
                dma((2 * groups, chips)), dma((2 * groups, chips)),
                dma((2 * groups, chips)), dma((2 * groups, chips)),
                dma((2 * groups, pieces)), dma((2 * groups, pieces)),
                dma((batches,)), dma((batches,)),
                dma((batches,)), dma((batches,)),
                dma((batches,)), dma((batches,)),
                dma((batches,)), dma((batches,)),
                dma((3,)), dma((3,)),
            ],
            compiler_params=pltpu.CompilerParams(collective_id=0, has_side_effects=True, vmem_limit_bytes=40000000),
        )(*[pltpu.with_memory_space_constraint(a, pltpu.HBM) for a in (sources, near_blocks, left_factors, right_factors)])

    return jax.shard_map(
        on_device,
        mesh=mesh,
        in_specs=(
            P("layer", None, "blk", None),
            P("layer", "blk", None),
            P("layer", "blk", None),
            P("layer", "blk", None),
        ),
        out_specs=P("layer", None, "blk", None),
        check_vma=False,
    )
```
